32 devices in a mesh: groups: 2 (over y), axial: 16 (over z, x, core).
Axes of the slice: x: 2, y: 2, z: 4, core: 2. Of those that a mesh axis runs over, the one named last changes fastest.
Arguments:
- pair_rep: bfloat16 [192, 96, 128], P(('groups', 'axial')), parts along dimension 0, may hold values from -6 to 6
- norm_out: float32 [128], replicated, may hold values from 0.5 to 1.5
- proj_out: bfloat16 [128, 512], replicated, may hold values from -0.5 to 0.5
- gate_out: bfloat16 [128, 128], replicated, may hold values from -0.5 to 0.5
- mid_out: float32 [128], replicated, may hold values from 0.5 to 1.5
- final_out: bfloat16 [128, 128], replicated, may hold values from -0.5 to 0.5
- norm_in: float32 [128], replicated, may hold values from 0.5 to 1.5
- proj_in: bfloat16 [128, 512], replicated, may hold values from -0.5 to 0.5
- gate_in: bfloat16 [128, 128], replicated, may hold values from -0.5 to 0.5
- mid_in: float32 [128], replicated, may hold values from 0.5 to 1.5
- final_in: bfloat16 [128, 128], replicated, may hold values from -0.5 to 0.5
Outputs:
- updated: bfloat16 [192, 96, 128], P(('groups', 'axial')), parts along dimension 0
The draws below stay inside these ranges and needn't reach their ends.
There are 2 independent parts, one for each index of `groups`. The reference program is written for one: setup_inputs(seed, part) draws one part's arguments, and reference() takes and returns one part's arrays. A program takes and returns all parts, laid end to end along the dimension named above; an argument that names none is the same for every part. Nothing has to cross between parts.
All inputs are finite; a program needn't handle non-finite values.
Results may differ from the reference program's by a relative error of at most 0.013.
Values may be sent and summed in bfloat16 or wider, within the bound.
A program may use at most 64 MiB of HBM per device.

```python
import math
import jax
import jax.numpy as jnp
from jax import lax

C = 128
HID = 128
N = 96


def levels(rng, shape, cuts, smallest, high):
    loudness = 1.0
    for dim, parts in cuts:
        heights = jax.random.uniform(jax.random.fold_in(jax.random.fold_in(rng, 6), dim), (parts,), jnp.float32, smallest / len(cuts), high / len(cuts))
        loudness = loudness * jnp.repeat(jnp.exp(heights), shape[dim] // parts).reshape((-1,) + (1,) * (len(shape) - 1 - dim))
    return loudness


def bell_draw(stream_key, shape, width, limit, shards=(), kind=jnp.bfloat16):
    drawn = jax.random.normal(stream_key, shape, jnp.float32) * width
    if len(shards) > 0:
        drawn = levels(stream_key, shape, shards, -0.22, 0.18) * drawn
    return jnp.clip(drawn, min=-limit, max=limit).astype(kind)


def setup_inputs(seed: int = 0, part: int = 0) -> dict:
    seeds = jax.random.split(jax.random.key(seed), 12)
    part_keys = jax.random.split(jax.random.fold_in(seeds[11], part), 12)
    pair_rep = bell_draw(part_keys[0], (N, N, C), 1.0, 6.0, ((0, 16),))
    norm_out = jnp.clip(1.0 + 0.1 * jax.random.normal(seeds[1], (C,), jnp.float32), 0.5, 1.5)
    proj_out = bell_draw(seeds[2], (C, 4 * HID), C ** -0.5, 0.5)
    gate_out = bell_draw(seeds[3], (C, C), C ** -0.5, 0.5)
    mid_out = jnp.clip(1.0 + 0.1 * jax.random.normal(seeds[4], (HID,), jnp.float32), 0.5, 1.5)
    final_out = bell_draw(seeds[5], (HID, C), HID ** -0.5, 0.5)
    norm_in = jnp.clip(1.0 + 0.1 * jax.random.normal(seeds[6], (C,), jnp.float32), 0.5, 1.5)
    proj_in = bell_draw(seeds[7], (C, 4 * HID), C ** -0.5, 0.5)
    gate_in = bell_draw(seeds[8], (C, C), C ** -0.5, 0.5)
    mid_in = jnp.clip(1.0 + 0.1 * jax.random.normal(seeds[9], (HID,), jnp.float32), 0.5, 1.5)
    final_in = bell_draw(seeds[10], (HID, C), HID ** -0.5, 0.5)
    return {"pair_rep": pair_rep, "norm_out": norm_out, "proj_out": proj_out, "gate_out": gate_out, "mid_out": mid_out, "final_out": final_out, "norm_in": norm_in, "proj_in": proj_in, "gate_in": gate_in, "mid_in": mid_in, "final_in": final_in}


EPS = 1e-05

def normalize(values, gain, axis):
    average = lax.optimization_barrier(jnp.mean(values, axis=axis, keepdims=True))
    spread = lax.optimization_barrier(jnp.mean(jnp.square(values - average), axis=axis, keepdims=True))
    return (values - average) * lax.rsqrt(spread + EPS) * gain

def project_rows(rows_in, norm_gain, weights):
    normed = normalize(rows_in.astype(jnp.float32), norm_gain, -1).astype(jnp.bfloat16)
    projected = jnp.einsum('rnc,ck->krn', normed.astype(jnp.float32), weights.astype(jnp.float32))
    hidden = weights.shape[1] // 4
    left_side = (jax.nn.sigmoid(projected[hidden:2 * hidden]) * projected[:hidden]).astype(jnp.bfloat16)
    right_side = (jax.nn.sigmoid(projected[3 * hidden:]) * projected[2 * hidden:3 * hidden]).astype(jnp.bfloat16)
    return (left_side, right_side, normed)

def triangle(left_side, right_side, outgoing):
    hidden = left_side.shape[0]
    extent = left_side.shape[1]
    group_size = math.gcd(hidden, 16)
    left_groups = left_side.reshape(hidden // group_size, group_size, extent, extent)
    right_groups = right_side.reshape(hidden // group_size, group_size, extent, extent)
    formula = 'kil,kjl->kij' if outgoing else 'kli,klj->kij'

    def one_group(operands):
        return jnp.einsum(formula, operands[0].astype(jnp.float32), operands[1].astype(jnp.float32)).astype(jnp.bfloat16)
    return lax.map(one_group, (left_groups, right_groups)).reshape(hidden, extent, extent)

def update(pair_rep, norm_gain, weights, gate_weight, mid_gain, final_weight, outgoing):
    extent = pair_rep.shape[0]
    channels = pair_rep.shape[2]
    hidden = weights.shape[1] // 4
    block_rows = math.gcd(extent, 64)
    block_count = extent // block_rows
    blocks = pair_rep.reshape(block_count, block_rows, extent, channels)
    left_side, right_side, normed = lax.map(lambda rows_in: project_rows(rows_in, norm_gain, weights), blocks)
    left_side = jnp.transpose(left_side, (1, 0, 2, 3)).reshape(hidden, extent, extent)
    right_side = jnp.transpose(right_side, (1, 0, 2, 3)).reshape(hidden, extent, extent)
    tri = triangle(left_side, right_side, outgoing)
    tri_blocks = jnp.transpose(tri.reshape(hidden, block_count, block_rows, extent), (1, 0, 2, 3))

    def finish(operands):
        rows_in, normed_rows, tri_rows = operands
        gating = jax.nn.sigmoid(jnp.einsum('rnc,ce->rne', normed_rows.astype(jnp.float32), gate_weight.astype(jnp.float32)))
        tri_normed = normalize(tri_rows.astype(jnp.float32), mid_gain[:, None, None], 0).astype(jnp.bfloat16)
        result = jnp.einsum('krn,kc->rnc', tri_normed.astype(jnp.float32), final_weight.astype(jnp.float32))
        return (rows_in.astype(jnp.float32) + gating * result).astype(jnp.bfloat16)
    return lax.map(finish, (blocks, normed, tri_blocks)).reshape(extent, extent, channels)

def reference(pair_rep, norm_out, proj_out, gate_out, mid_out, final_out, norm_in, proj_in, gate_in, mid_in, final_in):
    first = update(pair_rep, norm_out, proj_out, gate_out, mid_out, final_out, True)
    return update(first, norm_in, proj_in, gate_in, mid_in, final_in, False)
```

```python
import functools

import jax
import jax.numpy as jnp
from jax import lax
from jax.experimental import pallas as pl
from jax.experimental.pallas import tpu as pltpu
from jax.sharding import PartitionSpec as P

EPS = 1e-05


def normalize(values, gain, axis):
    average = jnp.mean(values, axis=axis, keepdims=True)
    spread = jnp.mean(jnp.square(values - average), axis=axis, keepdims=True)
    return (values - average) * lax.rsqrt(spread + EPS) * gain


def channel_product(left_side, right_side, outgoing):
    formula = "kil,kjl->kij" if outgoing else "kli,klj->kij"
    got_left, got_right = (
        lax.all_to_all(left_side, "axial", split_axis=0, concat_axis=1, tiled=True),
        lax.all_to_all(right_side, "axial", split_axis=0, concat_axis=1, tiled=True),
    )
    return jnp.einsum(formula, got_left, got_right, preferred_element_type=jnp.float32)


def update(pair_rep, norm_gain, weights, gate_weight, mid_gain, final_weight, outgoing):
    normed = normalize(pair_rep.astype(jnp.float32), norm_gain, -1).astype(jnp.bfloat16)
    projected = jnp.einsum("rnc,ck->krn", normed, weights, preferred_element_type=jnp.float32)
    hidden = weights.shape[1] // 4
    left_side = (jax.nn.sigmoid(projected[hidden : 2 * hidden]) * projected[:hidden]).astype(
        jnp.bfloat16
    )
    right_side = (
        jax.nn.sigmoid(projected[3 * hidden :]) * projected[2 * hidden : 3 * hidden]
    ).astype(jnp.bfloat16)
    product = channel_product(left_side, right_side, outgoing)
    tri = lax.all_to_all(
        product.astype(jnp.bfloat16), "axial", split_axis=1, concat_axis=0, tiled=True
    )
    gating = jax.nn.sigmoid(
        jnp.einsum("rnc,ce->rne", normed, gate_weight, preferred_element_type=jnp.float32)
    )
    tri_normed = normalize(tri.astype(jnp.float32), mid_gain[:, None, None], 0).astype(jnp.bfloat16)
    result = jnp.einsum("krn,kc->rnc", tri_normed, final_weight, preferred_element_type=jnp.float32)
    return (pair_rep.astype(jnp.float32) + gating * result).astype(jnp.bfloat16)


MESH = pl.DeviceIdType.MESH
CORES = 2
SIDES = 2
UP, DOWN, ACROSS, PEER = range(4)
VMEM_BYTES = 56 * 1024 * 1024


def fits(devices, pair_shape, proj_shape):
    rows, tokens, channels = pair_shape
    hidden = proj_shape[1] // 4
    held = 2 * devices * rows * tokens * hidden * 2
    work = 12 * rows * tokens * max(hidden, channels) * 4
    return (
        devices % (CORES * SIDES) == 0
        and devices * rows == tokens
        and rows <= 8
        and tokens % 16 == 0
        and channels == hidden
        and hidden % 128 == 0
        and held + work < VMEM_BYTES // 2
    )


def layer_norm(values, gain):
    average = jnp.mean(values, axis=-1, keepdims=True)
    centred = values - average
    spread = jnp.mean(jnp.square(centred), axis=-1, keepdims=True)
    return centred * lax.rsqrt(spread + EPS) * gain


def dot(left, right):
    return jnp.dot(left, right, preferred_element_type=jnp.float32)


def gather_kernel(
    devices,
    pair_ref,
    norm_out,
    proj_out,
    gate_out,
    mid_out,
    final_out,
    norm_in,
    proj_in,
    gate_in,
    mid_in,
    final_in,
    out_ref,
    held,
    columns_out,
    columns_in,
    columns_f32,
    rows_f32,
    left_f32,
    tri,
    gating,
    normed_ref,
    send_sem,
    recv_sem,
    columns_send_sem,
    columns_recv_sem,
):
    rows, tokens, channels = pair_ref.shape
    hidden = held.shape[-1]
    pad = 8
    length = devices // (CORES * SIDES)
    me = lax.axis_index("axial")
    core = me % CORES
    side = (me // CORES) % SIDES
    line = me // (CORES * SIDES)

    def index(at, on, of):
        return (at * SIDES + on) * CORES + of

    def near(step):
        if step == 0:
            return line
        low = jnp.minimum(line, length - 1 - line)
        first = jnp.where(2 * line < length, 1, -1)
        hop = (step + 1) // 2
        both = line - first * hop if step % 2 else line + first * hop
        alone = jnp.where(2 * line < length, step, length - 1 - step)
        return jnp.where(step <= 2 * low, both, alone)

    order = [near(step) for step in range(length)]
    mine = [index(at, side, core) for at in order]
    beside = [index(at, 1 - side, core) for at in order]
    peers = [index(at, side, 1 - core) for at in order]
    peers_beside = [index(at, 1 - side, 1 - core) for at in order]

    targets = {
        UP: index(jnp.minimum(line + 1, length - 1), side, core),
        DOWN: index(jnp.maximum(line - 1, 0), side, core),
        ACROSS: index(line, 1 - side, core),
        PEER: index(line, side, 1 - core),
    }

    def copy(phase, way, block):
        return pltpu.make_async_remote_copy(
            src_ref=held.at[phase, block],
            dst_ref=held.at[phase, block],
            send_sem=send_sem.at[phase, way, block],
            recv_sem=recv_sem.at[phase, block],
            device_id={"axial": targets[way]},
            device_id_type=MESH,
        )

    def along(phase, step, act):
        at, block = order[step], mine[step]

        @pl.when(jnp.logical_and(at <= line, line < length - 1))
        def _():
            act(copy(phase, UP, block))

        @pl.when(jnp.logical_and(at >= line, line > 0))
        def _():
            act(copy(phase, DOWN, block))

    def start(descriptor):
        descriptor.start()

    def finish_send(descriptor):
        descriptor.wait_send()

    def forward(phase, step):
        along(phase, step, start)
        copy(phase, ACROSS, mine[step]).start()
        copy(phase, PEER, mine[step]).start()

    def arrived(phase, block):
        copy(phase, PEER, block).wait_recv()

    def columns_copy(block, target):
        return pltpu.make_async_remote_copy(
            src_ref=columns_out.at[target],
            dst_ref=columns_in.at[block],
            send_sem=columns_send_sem.at[target],
            recv_sem=columns_recv_sem.at[block],
            device_id={"axial": target},
            device_id_type=MESH,
        )

    def exchange(phase, multiply):
        def from_line(step):
            arrived(phase, mine[step])
            forward(phase, step)

        def from_side(step):
            arrived(phase, beside[step])
            copy(phase, PEER, beside[step]).start()

        def from_peer(block):
            arrived(phase, block)
            multiply(block)

        multiply(mine[0])
        from_peer(peers[0])
        for step in range(1, length + 1):
            if step < length:
                from_line(step)
            from_side(step - 1)
            if step < length:
                multiply(mine[step])
            multiply(beside[step - 1])
            if step < length:
                from_peer(peers[step])
            from_peer(peers_beside[step - 1])

    def finish_sends(phase):
        for step in range(length):
            along(phase, step, finish_send)
            copy(phase, ACROSS, mine[step]).wait_send()
            copy(phase, PEER, mine[step]).wait_send()
            copy(phase, PEER, beside[step]).wait_send()

    def split(values):
        return values.reshape(rows, tokens, values.shape[-1])

    def gated(projected):
        return (jax.nn.sigmoid(projected[:, hidden:]) * projected[:, :hidden]).astype(jnp.bfloat16)

    def outgoing_block(block):
        def one(row, carry):
            right = held[0, block, row].astype(jnp.float32)
            total = jnp.sum(left_f32[...] * right[None], axis=1, keepdims=True)
            tri[:, pl.ds(block * rows + row, 1), :] = total
            return carry

        lax.fori_loop(0, rows, one, 0)

    def incoming_block(block):
        @pl.when(block != me)
        def _():
            columns_copy(block, targets[PEER]).wait_recv()

        rows_f32[...] = columns_in[block].astype(jnp.float32)

        def one(tile, carry):
            window = pl.ds(pl.multiple_of(tile * 16, 16), 16)
            right = held[1, block, :, window, :].astype(jnp.float32)
            for i in range(rows):
                total = tri[i, window, :]
                for l in range(rows):
                    total = total + rows_f32[pl.ds(l * pad + i, 1), :] * right[l]
                tri[i, window, :] = total
            return carry

        lax.fori_loop(0, tokens // 16, one, 0)

    def close(pair, mid_gain, final):
        product = tri[...].reshape(rows * tokens, hidden).astype(jnp.bfloat16).astype(jnp.float32)
        normed = layer_norm(product, mid_gain[...]).astype(jnp.bfloat16)
        return (pair + gating[...] * dot(normed, final[...])).astype(jnp.bfloat16)

    barrier = pltpu.get_barrier_semaphore()
    for offset in range(1, devices):
        pl.semaphore_signal(
            barrier,
            inc=1,
            device_id={"axial": lax.rem(me + offset, devices)},
            device_id_type=MESH,
        )

    pair = pair_ref[...].astype(jnp.float32).reshape(rows * tokens, channels)
    normed_ref[...] = layer_norm(pair, norm_out[...]).astype(jnp.bfloat16)
    held[0, me] = split(gated(dot(normed_ref[...], proj_out[:, 2 * hidden :])))
    pl.semaphore_wait(barrier, devices - 1)
    forward(0, 0)
    left_f32[...] = split(gated(dot(normed_ref[...], proj_out[:, : 2 * hidden]))).astype(jnp.float32)
    gating[...] = jax.nn.sigmoid(dot(normed_ref[...], gate_out[...]))
    exchange(0, outgoing_block)
    first = close(pair, mid_out, final_out).astype(jnp.float32)
    out_ref[...] = split(first).astype(jnp.bfloat16)

    normed_ref[...] = layer_norm(first, norm_in[...]).astype(jnp.bfloat16)
    held[1, me] = split(gated(dot(normed_ref[...], proj_in[:, 2 * hidden :])))
    forward(1, 0)
    left_f32[...] = split(gated(dot(normed_ref[...], proj_in[:, : 2 * hidden]))).astype(jnp.float32)
    columns_f32[...] = jnp.zeros_like(columns_f32)
    for target in range(devices):
        for l in range(rows):
            columns_f32[target, l * pad : l * pad + rows, :] = left_f32[
                l, target * rows : (target + 1) * rows, :
            ]
    columns_out[...] = columns_f32[...].astype(jnp.bfloat16)
    for offset in range(1, devices):
        columns_copy(me, lax.rem(me + offset, devices)).start()
    columns_in[me] = columns_out[me]
    gating[...] = jax.nn.sigmoid(dot(normed_ref[...], gate_in[...]))
    tri[...] = jnp.zeros_like(tri)
    exchange(1, incoming_block)
    again = out_ref[...].astype(jnp.float32).reshape(rows * tokens, channels)
    out_ref[...] = split(close(again, mid_in, final_in))

    for offset in range(1, devices):
        columns_copy(me, lax.rem(me + offset, devices)).wait_send()
    finish_sends(0)
    finish_sends(1)


def gather_rows(devices, pair_rep, *weights):
    rows, tokens, channels = pair_rep.shape
    hidden = weights[1].shape[1] // 4
    gains = [w.reshape(1, -1) if w.ndim == 1 else w for w in weights]
    packed = rows * 8
    return pl.pallas_call(
        functools.partial(gather_kernel, devices),
        out_shape=jax.ShapeDtypeStruct(pair_rep.shape, pair_rep.dtype),
        in_specs=[pl.BlockSpec(memory_space=pltpu.VMEM)] * 11,
        out_specs=pl.BlockSpec(memory_space=pltpu.VMEM),
        scratch_shapes=[
            pltpu.VMEM((2, devices, rows, tokens, hidden), jnp.bfloat16),
            pltpu.VMEM((devices, packed, hidden), jnp.bfloat16),
            pltpu.VMEM((devices, packed, hidden), jnp.bfloat16),
            pltpu.VMEM((devices, packed, hidden), jnp.float32),
            pltpu.VMEM((packed, hidden), jnp.float32),
            pltpu.VMEM((rows, tokens, hidden), jnp.float32),
            pltpu.VMEM((rows, tokens, hidden), jnp.float32),
            pltpu.VMEM((rows * tokens, channels), jnp.float32),
            pltpu.VMEM((rows * tokens, channels), jnp.bfloat16),
            pltpu.SemaphoreType.DMA((2, 4, devices)),
            pltpu.SemaphoreType.DMA((2, devices)),
            pltpu.SemaphoreType.DMA((devices,)),
            pltpu.SemaphoreType.DMA((devices,)),
        ],
        compiler_params=pltpu.CompilerParams(
            collective_id=0, has_side_effects=True, vmem_limit_bytes=VMEM_BYTES
        ),
        name="gather_rows",
    )(pair_rep, *gains)


def exchange_channels(
    pair_rep,
    norm_out,
    proj_out,
    gate_out,
    mid_out,
    final_out,
    norm_in,
    proj_in,
    gate_in,
    mid_in,
    final_in,
):
    first = update(pair_rep, norm_out, proj_out, gate_out, mid_out, final_out, True)
    return update(first, norm_in, proj_in, gate_in, mid_in, final_in, False)


def solution(mesh):
    devices = mesh.shape["axial"]

    def on_device(*arrays):
        if fits(devices, arrays[0].shape, arrays[2].shape):
            return gather_rows(devices, *arrays)
        return exchange_channels(*arrays)

    placed = (P(("groups", "axial"), None, None), P(), P(), P(), P(), P(), P(), P(), P(), P(), P())
    return jax.shard_map(
        on_device,
        mesh=mesh,
        in_specs=placed,
        out_specs=P(("groups", "axial"), None, None),
        check_vma=False,
    )
```

```python
import functools

import jax
import jax.numpy as jnp
from jax import lax
from jax.experimental import pallas as pl
from jax.experimental.pallas import tpu as pltpu
from jax.sharding import PartitionSpec as P

EPS = 1e-05


def normalize(values, gain, axis):
    average = jnp.mean(values, axis=axis, keepdims=True)
    spread = jnp.mean(jnp.square(values - average), axis=axis, keepdims=True)
    return (values - average) * lax.rsqrt(spread + EPS) * gain


def channel_product(left_side, right_side, outgoing):
    formula = "kil,kjl->kij" if outgoing else "kli,klj->kij"
    got_left, got_right = (
        lax.all_to_all(left_side, "axial", split_axis=0, concat_axis=1, tiled=True),
        lax.all_to_all(right_side, "axial", split_axis=0, concat_axis=1, tiled=True),
    )
    return jnp.einsum(formula, got_left, got_right, preferred_element_type=jnp.float32)


def update(pair_rep, norm_gain, weights, gate_weight, mid_gain, final_weight, outgoing):
    normed = normalize(pair_rep.astype(jnp.float32), norm_gain, -1).astype(jnp.bfloat16)
    projected = jnp.einsum("rnc,ck->krn", normed, weights, preferred_element_type=jnp.float32)
    hidden = weights.shape[1] // 4
    left_side = (jax.nn.sigmoid(projected[hidden : 2 * hidden]) * projected[:hidden]).astype(
        jnp.bfloat16
    )
    right_side = (
        jax.nn.sigmoid(projected[3 * hidden :]) * projected[2 * hidden : 3 * hidden]
    ).astype(jnp.bfloat16)
    product = channel_product(left_side, right_side, outgoing)
    tri = lax.all_to_all(
        product.astype(jnp.bfloat16), "axial", split_axis=1, concat_axis=0, tiled=True
    )
    gating = jax.nn.sigmoid(
        jnp.einsum("rnc,ce->rne", normed, gate_weight, preferred_element_type=jnp.float32)
    )
    tri_normed = normalize(tri.astype(jnp.float32), mid_gain[:, None, None], 0).astype(jnp.bfloat16)
    result = jnp.einsum("krn,kc->rnc", tri_normed, final_weight, preferred_element_type=jnp.float32)
    return (pair_rep.astype(jnp.float32) + gating * result).astype(jnp.bfloat16)


MESH = pl.DeviceIdType.MESH
CORES = 2
SIDES = 2
UP, DOWN, ACROSS = range(3)
VMEM_BYTES = 56 * 1024 * 1024


def fits(devices, pair_shape, proj_shape):
    rows, tokens, channels = pair_shape
    hidden = proj_shape[1] // 4
    held = 2 * devices * rows * tokens * hidden * 2
    work = 12 * rows * tokens * max(hidden, channels) * 4
    return (
        devices % (CORES * SIDES) == 0
        and devices * rows == tokens
        and rows <= 8
        and tokens % (16 * CORES) == 0
        and channels == hidden
        and hidden % 128 == 0
        and held + work < VMEM_BYTES // 2
    )


def layer_norm(values, gain):
    average = jnp.mean(values, axis=-1, keepdims=True)
    centred = values - average
    spread = jnp.mean(jnp.square(centred), axis=-1, keepdims=True)
    return centred * lax.rsqrt(spread + EPS) * gain


def dot(left, right):
    return jnp.dot(left, right, preferred_element_type=jnp.float32)


def gather_kernel(
    devices,
    pieces,
    pair_ref,
    norm_out,
    proj_out,
    gate_out,
    mid_out,
    final_out,
    norm_in,
    proj_in,
    gate_in,
    mid_in,
    final_in,
    out_ref,
    held,
    columns_out,
    columns_in,
    columns_f32,
    rows_f32,
    left_out,
    left_in,
    left_f32,
    partial,
    tri,
    part_out,
    part_in,
    gating,
    normed_ref,
    send_sem,
    recv_sem,
    columns_send_sem,
    columns_recv_sem,
    peer_send_sem,
    peer_recv_sem,
):
    rows, tokens, channels = pair_ref.shape
    hidden = held.shape[-1]
    chips = devices // CORES
    length = chips // SIDES
    both = CORES * rows
    pad = columns_out.shape[1] // rows
    share = chips * rows
    piece = rows // pieces
    me = lax.axis_index("axial")
    core = me % CORES
    chip = me // CORES
    side = chip % SIDES
    line = chip // SIDES
    low = jnp.minimum(line, length - 1 - line)

    def near(step):
        if step == 0:
            return line
        first = jnp.where(2 * line < length, 1, -1)
        hop = (step + 1) // 2
        pair = line - first * hop if step % 2 else line + first * hop
        alone = jnp.where(2 * line < length, step, length - 1 - step)
        return jnp.where(step <= 2 * low, pair, alone)

    def index(chip_at):
        return chip_at * CORES + core

    order = [near(step) for step in range(length)]
    mine = [at * SIDES + side for at in order]
    beside = [at * SIDES + 1 - side for at in order]
    peer = chip * CORES + 1 - core
    targets = {
        UP: index(jnp.minimum(line + 1, length - 1) * SIDES + side),
        DOWN: index(jnp.maximum(line - 1, 0) * SIDES + side),
        ACROSS: index(line * SIDES + 1 - side),
    }

    def line_event(event):
        step, part = 1 + event // pieces, event % pieces
        at = order[step]
        if event < 2 * pieces and length > 2:
            inner = low >= 1
            at = jnp.where(inner, order[1 + event % 2], at)
            part = jnp.where(inner, event // 2, part)
        return at, part

    def copy(phase, way, block, part):
        window = pl.ds(part * piece, piece)
        return pltpu.make_async_remote_copy(
            src_ref=held.at[phase, block, window],
            dst_ref=held.at[phase, block, window],
            send_sem=send_sem.at[phase, way, block, part],
            recv_sem=recv_sem.at[phase, block, part],
            device_id={"axial": targets[way]},
            device_id_type=MESH,
        )

    def pass_on(phase, at, part, act):
        block = at * SIDES + side

        @pl.when(jnp.logical_and(at <= line, line < length - 1))
        def _():
            act(copy(phase, UP, block, part))

        @pl.when(jnp.logical_and(at >= line, line > 0))
        def _():
            act(copy(phase, DOWN, block, part))

        act(copy(phase, ACROSS, block, part))

    def start(descriptor):
        descriptor.start()

    def finish_send(descriptor):
        descriptor.wait_send()

    def arrived(phase, block, part):
        copy(phase, ACROSS, block, part).wait_recv()

    def columns_copy(block, target):
        return pltpu.make_async_remote_copy(
            src_ref=columns_out.at[target],
            dst_ref=columns_in.at[block],
            send_sem=columns_send_sem.at[target],
            recv_sem=columns_recv_sem.at[block],
            device_id={"axial": index(target)},
            device_id_type=MESH,
        )

    def peer_copy(source, target, which):
        return pltpu.make_async_remote_copy(
            src_ref=source,
            dst_ref=target,
            send_sem=peer_send_sem.at[which],
            recv_sem=peer_recv_sem.at[which],
            device_id={"axial": peer},
            device_id_type=MESH,
        )

    left_copy = peer_copy(left_out, left_in, 0)
    tri_copy = peer_copy(part_out.at[0, :, :share], part_in.at[0, :, :share], 1)
    sum_copy = peer_copy(part_out.at[1], part_in.at[1], 2)

    def exchange(phase, multiply):
        def from_line(step):
            for event in range((step - 1) * pieces, step * pieces):
                at, part = line_event(event)
                arrived(phase, at * SIDES + side, part)
                pass_on(phase, at, part, start)

        def from_side(step):
            for part in range(pieces):
                arrived(phase, beside[step], part)
            multiply(beside[step])

        multiply(mine[0])
        if length > 1:
            from_line(1)
        from_side(0)
        for step in range(2, length):
            from_line(step)
            multiply(mine[step - 1])
            from_side(step - 1)
        if length > 1:
            multiply(mine[length - 1])
            from_side(length - 1)

    def finish_sends(phase):
        for step in range(length):
            for part in range(pieces):
                pass_on(phase, order[step], part, finish_send)

    def split(values):
        return values.reshape(rows, tokens, values.shape[-1])

    def gated(projected):
        return (jax.nn.sigmoid(projected[:, hidden:]) * projected[:, :hidden]).astype(jnp.bfloat16)

    def outgoing_block(block):
        def one(row, carry):
            right = held[0, block, row].astype(jnp.float32)
            at = pl.ds(block * rows + row, 1)
            for half in range(CORES):
                total = jnp.sum(left_f32[half] * right[None], axis=1, keepdims=True)
                partial[half, :, at, :] = total
            return carry

        lax.fori_loop(0, rows, one, 0)

    def incoming_block(block):
        @pl.when(block != chip)
        def _():
            columns_copy(block, chip * 0 + beside[0]).wait_recv()

        rows_f32[...] = columns_in[block].astype(jnp.float32)

        def one(tile, carry):
            window = pl.ds(pl.multiple_of(tile * 16, 16), 16)
            right = held[1, block, :, window, :].astype(jnp.float32)
            for i in range(both):
                total = partial[i // rows, i % rows, window, :]
                for l in range(rows):
                    total = total + rows_f32[pl.ds(l * pad + i, 1), :] * right[l]
                partial[i // rows, i % rows, window, :] = total
            return carry

        lax.fori_loop(0, tokens // 16, one, 0)

    def close(pair, mid_gain, final):
        product = tri[...].reshape(rows * tokens, hidden).astype(jnp.bfloat16).astype(jnp.float32)
        normed = layer_norm(product, mid_gain[...]).astype(jnp.bfloat16)
        return (pair + gating[...] * dot(normed, final[...])).astype(jnp.bfloat16)

    barrier = pltpu.get_barrier_semaphore()
    for offset in range(1, chips):
        pl.semaphore_signal(
            barrier,
            inc=1,
            device_id={"axial": index(lax.rem(chip + offset, chips))},
            device_id_type=MESH,
        )
    pl.semaphore_signal(barrier, inc=1, device_id={"axial": peer}, device_id_type=MESH)

    pair = pair_ref[...].astype(jnp.float32).reshape(rows * tokens, channels)
    normed_ref[...] = layer_norm(pair, norm_out[...]).astype(jnp.bfloat16)
    held[0, chip] = split(gated(dot(normed_ref[...], proj_out[:, 2 * hidden :])))
    pl.semaphore_wait(barrier, chips)
    for part in range(pieces):
        pass_on(0, line, part, start)
    left_out[...] = split(gated(dot(normed_ref[...], proj_out[:, : 2 * hidden])))
    left_copy.start()
    left_f32[0] = left_out[...].astype(jnp.float32)
    gating[...] = jax.nn.sigmoid(dot(normed_ref[...], gate_out[...]))
    left_copy.wait_recv()
    left_f32[1] = left_in[...].astype(jnp.float32)
    exchange(0, outgoing_block)
    part_out[0, :, :share] = partial[1, :, :share].astype(jnp.bfloat16)
    tri_copy.start()
    tri_copy.wait_recv()
    partial[1, :, :share] = part_in[0, :, :share].astype(jnp.float32)
    for half in range(CORES):
        for block in range(chips):
            at = (block * CORES + half) * rows
            got = pl.ds(block * rows, rows)
            tri[:, at : at + rows, :] = jnp.where(
                core == half, partial[0, :, got, :], partial[1, :, got, :]
            )
    first = close(pair, mid_out, final_out).astype(jnp.float32)
    out_ref[...] = split(first).astype(jnp.bfloat16)

    normed_ref[...] = layer_norm(first, norm_in[...]).astype(jnp.bfloat16)
    held[1, chip] = split(gated(dot(normed_ref[...], proj_in[:, 2 * hidden :])))
    for part in range(pieces):
        pass_on(1, line, part, start)
    left_f32[0] = split(gated(dot(normed_ref[...], proj_in[:, : 2 * hidden]))).astype(jnp.float32)
    columns_f32[...] = jnp.zeros_like(columns_f32)
    for target in range(chips):
        for l in range(rows):
            columns_f32[target, l * pad : l * pad + both, :] = left_f32[
                0, l, target * both : (target + 1) * both, :
            ]
    columns_out[...] = columns_f32[...].astype(jnp.bfloat16)
    for offset in range(1, chips):
        columns_copy(chip, lax.rem(chip + offset, chips)).start()
    columns_in[chip] = columns_out[chip]
    gating[...] = jax.nn.sigmoid(dot(normed_ref[...], gate_in[...]))
    partial[...] = jnp.zeros_like(partial)
    exchange(1, incoming_block)
    part_out[1] = partial[1 - core].astype(jnp.bfloat16)
    sum_copy.start()
    sum_copy.wait_recv()
    tri[...] = partial[core] + part_in[1].astype(jnp.float32)
    again = out_ref[...].astype(jnp.float32).reshape(rows * tokens, channels)
    out_ref[...] = split(close(again, mid_in, final_in))

    for offset in range(1, chips):
        columns_copy(chip, lax.rem(chip + offset, chips)).wait_send()
    left_copy.wait_send()
    tri_copy.wait_send()
    sum_copy.wait_send()
    finish_sends(0)
    finish_sends(1)


def gather_rows(devices, pair_rep, *weights):
    rows, tokens, channels = pair_rep.shape
    hidden = weights[1].shape[1] // 4
    gains = [w.reshape(1, -1) if w.ndim == 1 else w for w in weights]
    chips = devices // CORES
    packed = rows * (-(-CORES * rows // 8) * 8)
    pieces = 2 if rows % 2 == 0 else 1
    block = (rows, tokens, hidden)
    return pl.pallas_call(
        functools.partial(gather_kernel, devices, pieces),
        out_shape=jax.ShapeDtypeStruct(pair_rep.shape, pair_rep.dtype),
        in_specs=[pl.BlockSpec(memory_space=pltpu.VMEM)] * 11,
        out_specs=pl.BlockSpec(memory_space=pltpu.VMEM),
        scratch_shapes=[
            pltpu.VMEM((2, chips) + block, jnp.bfloat16),
            pltpu.VMEM((chips, packed, hidden), jnp.bfloat16),
            pltpu.VMEM((chips, packed, hidden), jnp.bfloat16),
            pltpu.VMEM((chips, packed, hidden), jnp.float32),
            pltpu.VMEM((packed, hidden), jnp.float32),
            pltpu.VMEM(block, jnp.bfloat16),
            pltpu.VMEM(block, jnp.bfloat16),
            pltpu.VMEM((CORES,) + block, jnp.float32),
            pltpu.VMEM((CORES,) + block, jnp.float32),
            pltpu.VMEM(block, jnp.float32),
            pltpu.VMEM((2,) + block, jnp.bfloat16),
            pltpu.VMEM((2,) + block, jnp.bfloat16),
            pltpu.VMEM((rows * tokens, channels), jnp.float32),
            pltpu.VMEM((rows * tokens, channels), jnp.bfloat16),
            pltpu.SemaphoreType.DMA((2, 3, chips, pieces)),
            pltpu.SemaphoreType.DMA((2, chips, pieces)),
            pltpu.SemaphoreType.DMA((chips,)),
            pltpu.SemaphoreType.DMA((chips,)),
            pltpu.SemaphoreType.DMA((3,)),
            pltpu.SemaphoreType.DMA((3,)),
        ],
        compiler_params=pltpu.CompilerParams(
            collective_id=0, has_side_effects=True, vmem_limit_bytes=VMEM_BYTES
        ),
        name="gather_rows",
    )(pair_rep, *gains)


def exchange_channels(
    pair_rep,
    norm_out,
    proj_out,
    gate_out,
    mid_out,
    final_out,
    norm_in,
    proj_in,
    gate_in,
    mid_in,
    final_in,
):
    first = update(pair_rep, norm_out, proj_out, gate_out, mid_out, final_out, True)
    return update(first, norm_in, proj_in, gate_in, mid_in, final_in, False)


def solution(mesh):
    devices = mesh.shape["axial"]

    def on_device(*arrays):
        if fits(devices, arrays[0].shape, arrays[2].shape):
            return gather_rows(devices, *arrays)
        return exchange_channels(*arrays)

    placed = (P(("groups", "axial"), None, None), P(), P(), P(), P(), P(), P(), P(), P(), P(), P())
    return jax.shard_map(
        on_device,
        mesh=mesh,
        in_specs=placed,
        out_specs=P(("groups", "axial"), None, None),
        check_vma=False,
    )
```

```python
import functools

import jax
import jax.numpy as jnp
from jax import lax
from jax.experimental import pallas as pl
from jax.experimental.pallas import tpu as pltpu
from jax.sharding import PartitionSpec as P

EPS = 1e-05


def normalize(values, gain, axis):
    average = jnp.mean(values, axis=axis, keepdims=True)
    spread = jnp.mean(jnp.square(values - average), axis=axis, keepdims=True)
    return (values - average) * lax.rsqrt(spread + EPS) * gain


def channel_product(left_side, right_side, outgoing):
    formula = "kil,kjl->kij" if outgoing else "kli,klj->kij"
    got_left, got_right = (
        lax.all_to_all(left_side, "axial", split_axis=0, concat_axis=1, tiled=True),
        lax.all_to_all(right_side, "axial", split_axis=0, concat_axis=1, tiled=True),
    )
    return jnp.einsum(formula, got_left, got_right, preferred_element_type=jnp.float32)


def update(pair_rep, norm_gain, weights, gate_weight, mid_gain, final_weight, outgoing):
    normed = normalize(pair_rep.astype(jnp.float32), norm_gain, -1).astype(jnp.bfloat16)
    projected = jnp.einsum("rnc,ck->krn", normed, weights, preferred_element_type=jnp.float32)
    hidden = weights.shape[1] // 4
    left_side = (jax.nn.sigmoid(projected[hidden : 2 * hidden]) * projected[:hidden]).astype(
        jnp.bfloat16
    )
    right_side = (
        jax.nn.sigmoid(projected[3 * hidden :]) * projected[2 * hidden : 3 * hidden]
    ).astype(jnp.bfloat16)
    product = channel_product(left_side, right_side, outgoing)
    tri = lax.all_to_all(
        product.astype(jnp.bfloat16), "axial", split_axis=1, concat_axis=0, tiled=True
    )
    gating = jax.nn.sigmoid(
        jnp.einsum("rnc,ce->rne", normed, gate_weight, preferred_element_type=jnp.float32)
    )
    tri_normed = normalize(tri.astype(jnp.float32), mid_gain[:, None, None], 0).astype(jnp.bfloat16)
    result = jnp.einsum("krn,kc->rnc", tri_normed, final_weight, preferred_element_type=jnp.float32)
    return (pair_rep.astype(jnp.float32) + gating * result).astype(jnp.bfloat16)


MESH = pl.DeviceIdType.MESH
CORES = 2
SIDES = 2
UP, DOWN, ACROSS = range(3)
VMEM_BYTES = 56 * 1024 * 1024


def fits(devices, pair_shape, proj_shape):
    rows, tokens, channels = pair_shape
    hidden = proj_shape[1] // 4
    held = 2 * devices * rows * tokens * hidden * 2
    work = 12 * rows * tokens * max(hidden, channels) * 4
    return (
        devices % (CORES * SIDES) == 0
        and devices * rows == tokens
        and rows <= 8
        and tokens % (16 * CORES) == 0
        and channels == hidden
        and hidden % 128 == 0
        and held + work < VMEM_BYTES // 2
    )


def layer_norm(values, gain):
    average = jnp.mean(values, axis=-1, keepdims=True)
    centred = values - average
    spread = jnp.mean(jnp.square(centred), axis=-1, keepdims=True)
    return centred * lax.rsqrt(spread + EPS) * gain


def dot(left, right):
    return jnp.dot(left, right, preferred_element_type=jnp.float32)


def gather_kernel(
    devices,
    pieces,
    pair_ref,
    norm_out,
    proj_out,
    gate_out,
    mid_out,
    final_out,
    norm_in,
    proj_in,
    gate_in,
    mid_in,
    final_in,
    out_ref,
    held,
    columns_out,
    columns_in,
    columns_f32,
    rows_f32,
    left_out,
    left_in,
    left_f32,
    partial,
    tri,
    part_out,
    part_in,
    gating,
    normed_ref,
    send_sem,
    recv_sem,
    columns_send_sem,
    columns_recv_sem,
    peer_send_sem,
    peer_recv_sem,
):
    rows, tokens, channels = pair_ref.shape
    hidden = held.shape[-1]
    chips = devices // CORES
    length = chips // SIDES
    both = CORES * rows
    pad = columns_out.shape[1] // rows
    share = chips * rows
    piece = rows // pieces
    me = lax.axis_index("axial")
    core = me % CORES
    chip = me // CORES
    side = chip % SIDES
    line = chip // SIDES
    low = jnp.minimum(line, length - 1 - line)

    def near(step):
        if step == 0:
            return line
        first = jnp.where(2 * line < length, 1, -1)
        hop = (step + 1) // 2
        pair = line - first * hop if step % 2 else line + first * hop
        alone = jnp.where(2 * line < length, step, length - 1 - step)
        return jnp.where(step <= 2 * low, pair, alone)

    def index(chip_at):
        return chip_at * CORES + core

    order = [near(step) for step in range(length)]
    mine = [at * SIDES + side for at in order]
    beside = [at * SIDES + 1 - side for at in order]
    peer = chip * CORES + 1 - core
    targets = {
        UP: index(jnp.minimum(line + 1, length - 1) * SIDES + side),
        DOWN: index(jnp.maximum(line - 1, 0) * SIDES + side),
        ACROSS: index(line * SIDES + 1 - side),
    }

    def line_event(event):
        step, part = 1 + event // pieces, event % pieces
        at = order[step]
        if event < 2 * pieces and length > 2:
            inner = low >= 1
            at = jnp.where(inner, order[1 + event % 2], at)
            part = jnp.where(inner, event // 2, part)
        return at, part

    def copy(phase, way, block, part):
        window = pl.ds(part * piece, piece)
        return pltpu.make_async_remote_copy(
            src_ref=held.at[phase, block, window],
            dst_ref=held.at[phase, block, window],
            send_sem=send_sem.at[phase, way, block, part],
            recv_sem=recv_sem.at[phase, block, part],
            device_id={"axial": targets[way]},
            device_id_type=MESH,
        )

    def pass_on(phase, at, part, act):
        block = at * SIDES + side

        @pl.when(jnp.logical_and(at <= line, line < length - 1))
        def _():
            act(copy(phase, UP, block, part))

        @pl.when(jnp.logical_and(at >= line, line > 0))
        def _():
            act(copy(phase, DOWN, block, part))

        act(copy(phase, ACROSS, block, part))

    def start(descriptor):
        descriptor.start()

    def finish_send(descriptor):
        descriptor.wait_send()

    def arrived(phase, block, part):
        copy(phase, ACROSS, block, part).wait_recv()

    def columns_copy(block, target):
        return pltpu.make_async_remote_copy(
            src_ref=columns_out.at[target],
            dst_ref=columns_in.at[block],
            send_sem=columns_send_sem.at[target],
            recv_sem=columns_recv_sem.at[block],
            device_id={"axial": index(target)},
            device_id_type=MESH,
        )

    def peer_copy(source, target, which):
        return pltpu.make_async_remote_copy(
            src_ref=source,
            dst_ref=target,
            send_sem=peer_send_sem.at[which],
            recv_sem=peer_recv_sem.at[which],
            device_id={"axial": peer},
            device_id_type=MESH,
        )

    left_copy = peer_copy(left_out, left_in, 0)
    tri_copy = peer_copy(part_out.at[0, :, :share], part_in.at[0, :, :share], 1)
    sum_copy = peer_copy(part_out.at[1], part_in.at[1], 2)

    def exchange(phase, multiply):
        def from_line(step):
            for event in range((step - 1) * pieces, step * pieces):
                at, part = line_event(event)
                arrived(phase, at * SIDES + side, part)
                pass_on(phase, at, part, start)

        def from_side(step):
            for part in range(pieces):
                arrived(phase, beside[step], part)
            multiply(beside[step])

        multiply(mine[0])
        for step in range(1, length):
            from_line(step)
            if step == 2:
                from_side(0)
            if 2 <= step < length - 1:
                multiply(mine[step - 1])
        for step in range(max(1, length - 2), length):
            multiply(mine[step])
        for step in range(1 if length > 2 else 0, length):
            from_side(step)

    def finish_sends(phase):
        for step in range(length):
            for part in range(pieces):
                pass_on(phase, order[step], part, finish_send)

    def split(values):
        return values.reshape(rows, tokens, values.shape[-1])

    def gated(projected):
        return (jax.nn.sigmoid(projected[:, hidden:]) * projected[:, :hidden]).astype(jnp.bfloat16)

    def outgoing_block(block):
        def one(row, carry):
            right = held[0, block, row].astype(jnp.float32)
            at = pl.ds(block * rows + row, 1)
            for half in range(CORES):
                total = jnp.sum(left_f32[half] * right[None], axis=1, keepdims=True)
                partial[half, :, at, :] = total
            return carry

        lax.fori_loop(0, rows, one, 0)

    def incoming_block(block):
        @pl.when(block != chip)
        def _():
            columns_copy(block, chip * 0 + beside[0]).wait_recv()

        rows_f32[...] = columns_in[block].astype(jnp.float32)

        def one(tile, carry):
            window = pl.ds(pl.multiple_of(tile * 16, 16), 16)
            right = held[1, block, :, window, :].astype(jnp.float32)
            for i in range(both):
                total = partial[i // rows, i % rows, window, :]
                for l in range(rows):
                    total = total + rows_f32[pl.ds(l * pad + i, 1), :] * right[l]
                partial[i // rows, i % rows, window, :] = total
            return carry

        lax.fori_loop(0, tokens // 16, one, 0)

    def close(pair, mid_gain, final):
        product = tri[...].reshape(rows * tokens, hidden).astype(jnp.bfloat16).astype(jnp.float32)
        normed = layer_norm(product, mid_gain[...]).astype(jnp.bfloat16)
        return (pair + gating[...] * dot(normed, final[...])).astype(jnp.bfloat16)

    barrier = pltpu.get_barrier_semaphore()
    for offset in range(1, chips):
        pl.semaphore_signal(
            barrier,
            inc=1,
            device_id={"axial": index(lax.rem(chip + offset, chips))},
            device_id_type=MESH,
        )
    pl.semaphore_signal(barrier, inc=1, device_id={"axial": peer}, device_id_type=MESH)

    pair = pair_ref[...].astype(jnp.float32).reshape(rows * tokens, channels)
    normed_ref[...] = layer_norm(pair, norm_out[...]).astype(jnp.bfloat16)
    held[0, chip] = split(gated(dot(normed_ref[...], proj_out[:, 2 * hidden :])))
    pl.semaphore_wait(barrier, chips)
    for part in range(pieces):
        pass_on(0, line, part, start)
    left_out[...] = split(gated(dot(normed_ref[...], proj_out[:, : 2 * hidden])))
    left_copy.start()
    left_f32[0] = left_out[...].astype(jnp.float32)
    gating[...] = jax.nn.sigmoid(dot(normed_ref[...], gate_out[...]))
    left_copy.wait_recv()
    left_f32[1] = left_in[...].astype(jnp.float32)
    exchange(0, outgoing_block)
    part_out[0, :, :share] = partial[1, :, :share].astype(jnp.bfloat16)
    tri_copy.start()
    tri_copy.wait_recv()
    partial[1, :, :share] = part_in[0, :, :share].astype(jnp.float32)
    for half in range(CORES):
        for block in range(chips):
            at = (block * CORES + half) * rows
            got = pl.ds(block * rows, rows)
            tri[:, at : at + rows, :] = jnp.where(
                core == half, partial[0, :, got, :], partial[1, :, got, :]
            )
    first = close(pair, mid_out, final_out).astype(jnp.float32)
    out_ref[...] = split(first).astype(jnp.bfloat16)

    normed_ref[...] = layer_norm(first, norm_in[...]).astype(jnp.bfloat16)
    held[1, chip] = split(gated(dot(normed_ref[...], proj_in[:, 2 * hidden :])))
    for part in range(pieces):
        pass_on(1, line, part, start)
    left_f32[0] = split(gated(dot(normed_ref[...], proj_in[:, : 2 * hidden]))).astype(jnp.float32)
    columns_f32[...] = jnp.zeros_like(columns_f32)
    for target in range(chips):
        for l in range(rows):
            columns_f32[target, l * pad : l * pad + both, :] = left_f32[
                0, l, target * both : (target + 1) * both, :
            ]
    columns_out[...] = columns_f32[...].astype(jnp.bfloat16)
    for offset in range(1, chips):
        columns_copy(chip, lax.rem(chip + offset, chips)).start()
    columns_in[chip] = columns_out[chip]
    gating[...] = jax.nn.sigmoid(dot(normed_ref[...], gate_in[...]))
    partial[...] = jnp.zeros_like(partial)
    exchange(1, incoming_block)
    part_out[1] = partial[1 - core].astype(jnp.bfloat16)
    sum_copy.start()
    sum_copy.wait_recv()
    tri[...] = partial[core] + part_in[1].astype(jnp.float32)
    again = out_ref[...].astype(jnp.float32).reshape(rows * tokens, channels)
    out_ref[...] = split(close(again, mid_in, final_in))

    for offset in range(1, chips):
        columns_copy(chip, lax.rem(chip + offset, chips)).wait_send()
    left_copy.wait_send()
    tri_copy.wait_send()
    sum_copy.wait_send()
    finish_sends(0)
    finish_sends(1)


def gather_rows(devices, pair_rep, *weights):
    rows, tokens, channels = pair_rep.shape
    hidden = weights[1].shape[1] // 4
    gains = [w.reshape(1, -1) if w.ndim == 1 else w for w in weights]
    chips = devices // CORES
    packed = rows * (-(-CORES * rows // 8) * 8)
    pieces = 2 if rows % 2 == 0 else 1
    block = (rows, tokens, hidden)
    return pl.pallas_call(
        functools.partial(gather_kernel, devices, pieces),
        out_shape=jax.ShapeDtypeStruct(pair_rep.shape, pair_rep.dtype),
        in_specs=[pl.BlockSpec(memory_space=pltpu.VMEM)] * 11,
        out_specs=pl.BlockSpec(memory_space=pltpu.VMEM),
        scratch_shapes=[
            pltpu.VMEM((2, chips) + block, jnp.bfloat16),
            pltpu.VMEM((chips, packed, hidden), jnp.bfloat16),
            pltpu.VMEM((chips, packed, hidden), jnp.bfloat16),
            pltpu.VMEM((chips, packed, hidden), jnp.float32),
            pltpu.VMEM((packed, hidden), jnp.float32),
            pltpu.VMEM(block, jnp.bfloat16),
            pltpu.VMEM(block, jnp.bfloat16),
            pltpu.VMEM((CORES,) + block, jnp.float32),
            pltpu.VMEM((CORES,) + block, jnp.float32),
            pltpu.VMEM(block, jnp.float32),
            pltpu.VMEM((2,) + block, jnp.bfloat16),
            pltpu.VMEM((2,) + block, jnp.bfloat16),
            pltpu.VMEM((rows * tokens, channels), jnp.float32),
            pltpu.VMEM((rows * tokens, channels), jnp.bfloat16),
            pltpu.SemaphoreType.DMA((2, 3, chips, pieces)),
            pltpu.SemaphoreType.DMA((2, chips, pieces)),
            pltpu.SemaphoreType.DMA((chips,)),
            pltpu.SemaphoreType.DMA((chips,)),
            pltpu.SemaphoreType.DMA((3,)),
            pltpu.SemaphoreType.DMA((3,)),
        ],
        compiler_params=pltpu.CompilerParams(
            collective_id=0, has_side_effects=True, vmem_limit_bytes=VMEM_BYTES
        ),
        name="gather_rows",
    )(pair_rep, *gains)


def exchange_channels(
    pair_rep,
    norm_out,
    proj_out,
    gate_out,
    mid_out,
    final_out,
    norm_in,
    proj_in,
    gate_in,
    mid_in,
    final_in,
):
    first = update(pair_rep, norm_out, proj_out, gate_out, mid_out, final_out, True)
    return update(first, norm_in, proj_in, gate_in, mid_in, final_in, False)


def solution(mesh):
    devices = mesh.shape["axial"]

    def on_device(*arrays):
        if fits(devices, arrays[0].shape, arrays[2].shape):
            return gather_rows(devices, *arrays)
        return exchange_channels(*arrays)

    placed = (P(("groups", "axial"), None, None), P(), P(), P(), P(), P(), P(), P(), P(), P(), P())
    return jax.shard_map(
        on_device,
        mesh=mesh,
        in_specs=placed,
        out_specs=P(("groups", "axial"), None, None),
        check_vma=False,
    )
```

```python
import functools

import jax
import jax.numpy as jnp
from jax import lax
from jax.experimental import pallas as pl
from jax.experimental.pallas import tpu as pltpu
from jax.sharding import PartitionSpec as P

EPS = 1e-05


def normalize(values, gain, axis):
    average = jnp.mean(values, axis=axis, keepdims=True)
    spread = jnp.mean(jnp.square(values - average), axis=axis, keepdims=True)
    return (values - average) * lax.rsqrt(spread + EPS) * gain


def channel_product(left_side, right_side, outgoing):
    formula = "kil,kjl->kij" if outgoing else "kli,klj->kij"
    got_left, got_right = (
        lax.all_to_all(left_side, "axial", split_axis=0, concat_axis=1, tiled=True),
        lax.all_to_all(right_side, "axial", split_axis=0, concat_axis=1, tiled=True),
    )
    return jnp.einsum(formula, got_left, got_right, preferred_element_type=jnp.float32)


def update(pair_rep, norm_gain, weights, gate_weight, mid_gain, final_weight, outgoing):
    normed = normalize(pair_rep.astype(jnp.float32), norm_gain, -1).astype(jnp.bfloat16)
    projected = jnp.einsum("rnc,ck->krn", normed, weights, preferred_element_type=jnp.float32)
    hidden = weights.shape[1] // 4
    left_side = (jax.nn.sigmoid(projected[hidden : 2 * hidden]) * projected[:hidden]).astype(
        jnp.bfloat16
    )
    right_side = (
        jax.nn.sigmoid(projected[3 * hidden :]) * projected[2 * hidden : 3 * hidden]
    ).astype(jnp.bfloat16)
    product = channel_product(left_side, right_side, outgoing)
    tri = lax.all_to_all(
        product.astype(jnp.bfloat16), "axial", split_axis=1, concat_axis=0, tiled=True
    )
    gating = jax.nn.sigmoid(
        jnp.einsum("rnc,ce->rne", normed, gate_weight, preferred_element_type=jnp.float32)
    )
    tri_normed = normalize(tri.astype(jnp.float32), mid_gain[:, None, None], 0).astype(jnp.bfloat16)
    result = jnp.einsum("krn,kc->rnc", tri_normed, final_weight, preferred_element_type=jnp.float32)
    return (pair_rep.astype(jnp.float32) + gating * result).astype(jnp.bfloat16)


MESH = pl.DeviceIdType.MESH
CORES = 2
SIDES = 2
UP, DOWN, ACROSS = range(3)
VMEM_BYTES = 56 * 1024 * 1024


def fits(devices, pair_shape, proj_shape):
    rows, tokens, channels = pair_shape
    hidden = proj_shape[1] // 4
    held = 2 * devices * rows * tokens * hidden * 2
    work = 12 * rows * tokens * max(hidden, channels) * 4
    return (
        devices % (CORES * SIDES) == 0
        and devices * rows == tokens
        and rows <= 8
        and tokens % (16 * CORES) == 0
        and channels == hidden
        and hidden % 128 == 0
        and held + work < VMEM_BYTES // 2
    )


def layer_norm(values, gain):
    average = jnp.mean(values, axis=-1, keepdims=True)
    centred = values - average
    spread = jnp.mean(jnp.square(centred), axis=-1, keepdims=True)
    return centred * lax.rsqrt(spread + EPS) * gain


def dot(left, right):
    return jnp.dot(left, right, preferred_element_type=jnp.float32)


def gather_kernel(
    devices,
    pieces,
    pair_ref,
    norm_out,
    proj_out,
    gate_out,
    mid_out,
    final_out,
    norm_in,
    proj_in,
    gate_in,
    mid_in,
    final_in,
    out_ref,
    held,
    columns_out,
    columns_in,
    columns_f32,
    rows_f32,
    left_out,
    left_in,
    left_f32,
    partial,
    tri,
    part_out,
    part_in,
    gating,
    normed_ref,
    send_sem,
    recv_sem,
    columns_send_sem,
    columns_recv_sem,
    peer_send_sem,
    peer_recv_sem,
):
    rows, tokens, channels = pair_ref.shape
    hidden = held.shape[-1]
    chips = devices // CORES
    length = chips // SIDES
    both = CORES * rows
    pad = both
    share = chips * rows
    piece = rows // pieces
    me = lax.axis_index("axial")
    core = me % CORES
    chip = me // CORES
    side = chip % SIDES
    line = chip // SIDES
    low = jnp.minimum(line, length - 1 - line)

    def near(step):
        if step == 0:
            return line
        first = jnp.where(2 * line < length, 1, -1)
        hop = (step + 1) // 2
        pair = line - first * hop if step % 2 else line + first * hop
        alone = jnp.where(2 * line < length, step, length - 1 - step)
        return jnp.where(step <= 2 * low, pair, alone)

    def index(chip_at):
        return chip_at * CORES + core

    order = [near(step) for step in range(length)]
    mine = [at * SIDES + side for at in order]
    beside = [at * SIDES + 1 - side for at in order]
    peer = chip * CORES + 1 - core
    targets = {
        UP: index(jnp.minimum(line + 1, length - 1) * SIDES + side),
        DOWN: index(jnp.maximum(line - 1, 0) * SIDES + side),
        ACROSS: index(line * SIDES + 1 - side),
    }

    def line_event(event):
        step, part = 1 + event // pieces, event % pieces
        at = order[step]
        if event < 2 * pieces and length > 2:
            inner = low >= 1
            at = jnp.where(inner, order[1 + event % 2], at)
            part = jnp.where(inner, event // 2, part)
        return at, part

    def copy(phase, way, block, part):
        window = pl.ds(part * piece, piece)
        return pltpu.make_async_remote_copy(
            src_ref=held.at[phase, block, window],
            dst_ref=held.at[phase, block, window],
            send_sem=send_sem.at[phase, way, block, part],
            recv_sem=recv_sem.at[phase, block, part],
            device_id={"axial": targets[way]},
            device_id_type=MESH,
        )

    def pass_on(phase, at, part, act):
        block = at * SIDES + side

        @pl.when(jnp.logical_and(at <= line, line < length - 1))
        def _():
            act(copy(phase, UP, block, part))

        @pl.when(jnp.logical_and(at >= line, line > 0))
        def _():
            act(copy(phase, DOWN, block, part))

        act(copy(phase, ACROSS, block, part))

    def start(descriptor):
        descriptor.start()

    def finish_send(descriptor):
        descriptor.wait_send()

    def arrived(phase, block, part):
        copy(phase, ACROSS, block, part).wait_recv()

    def columns_copy(block, target):
        return pltpu.make_async_remote_copy(
            src_ref=columns_out.at[target],
            dst_ref=columns_in.at[block],
            send_sem=columns_send_sem.at[target],
            recv_sem=columns_recv_sem.at[block],
            device_id={"axial": index(target)},
            device_id_type=MESH,
        )

    def peer_copy(source, target, which):
        return pltpu.make_async_remote_copy(
            src_ref=source,
            dst_ref=target,
            send_sem=peer_send_sem.at[which],
            recv_sem=peer_recv_sem.at[which],
            device_id={"axial": peer},
            device_id_type=MESH,
        )

    left_copy = peer_copy(left_out, left_in, 0)
    tri_copy = peer_copy(part_out.at[0, :, :share], part_in.at[0, :, :share], 1)
    sum_copy = peer_copy(part_out.at[1], part_in.at[1], 2)

    def exchange(phase, multiply):
        def from_line(step):
            for event in range((step - 1) * pieces, step * pieces):
                at, part = line_event(event)
                arrived(phase, at * SIDES + side, part)
                pass_on(phase, at, part, start)

        def from_side(step):
            for part in range(pieces):
                arrived(phase, beside[step], part)
            multiply(beside[step])

        multiply(mine[0])
        for step in range(1, length):
            from_line(step)
            if step == 2:
                from_side(0)
            if 2 <= step < length - 1:
                multiply(mine[step - 1])
        for step in range(max(1, length - 2), length):
            multiply(mine[step])
        for step in range(1 if length > 2 else 0, length):
            from_side(step)

    def finish_sends(phase):
        for step in range(length):
            for part in range(pieces):
                pass_on(phase, order[step], part, finish_send)

    def split(values):
        return values.reshape(rows, tokens, values.shape[-1])

    def gated(projected):
        return (jax.nn.sigmoid(projected[:, hidden:]) * projected[:, :hidden]).astype(jnp.bfloat16)

    def outgoing_block(block):
        def one(row, carry):
            right = held[0, block, row].astype(jnp.float32)
            at = pl.ds(block * rows + row, 1)
            for half in range(CORES):
                total = jnp.sum(left_f32[half] * right[None], axis=1, keepdims=True)
                partial[half, :, at, :] = total
            return carry

        lax.fori_loop(0, rows, one, 0)

    def incoming_block(block):
        @pl.when(block != chip)
        def _():
            columns_copy(block, chip * 0 + beside[0]).wait_recv()

        rows_f32[...] = columns_in[block].astype(jnp.float32)

        def one(tile, carry):
            window = pl.ds(pl.multiple_of(tile * 16, 16), 16)
            right = held[1, block, :, window, :].astype(jnp.float32)
            for i in range(both):
                total = partial[i // rows, i % rows, window, :]
                for l in range(rows):
                    total = total + rows_f32[pl.ds(l * pad + i, 1), :] * right[l]
                partial[i // rows, i % rows, window, :] = total
            return carry

        lax.fori_loop(0, tokens // 16, one, 0)

    def flat(values):
        return values.reshape(-1, values.shape[-1])

    def close(pair, part, mid_gain, final):
        product = flat(tri[span(part)]).astype(jnp.bfloat16).astype(jnp.float32)
        normed = layer_norm(product, mid_gain[...]).astype(jnp.bfloat16)
        return (pair + gating[flat_span(part)] * dot(normed, final[...])).astype(jnp.bfloat16)

    def span(part):
        return pl.ds(part * piece, piece)

    def flat_span(part):
        return pl.ds(part * piece * tokens, piece * tokens)

    def open_piece(phase, part, pair, norm, proj):
        normed = layer_norm(pair, norm[...]).astype(jnp.bfloat16)
        normed_ref[flat_span(part)] = normed
        right = gated(dot(normed, proj[:, 2 * hidden :]))
        held[phase, chip, span(part)] = right.reshape(piece, tokens, hidden)

    barrier = pltpu.get_barrier_semaphore()
    for offset in range(1, chips):
        pl.semaphore_signal(
            barrier,
            inc=1,
            device_id={"axial": index(lax.rem(chip + offset, chips))},
            device_id_type=MESH,
        )
    pl.semaphore_signal(barrier, inc=1, device_id={"axial": peer}, device_id_type=MESH)

    for part in range(pieces):
        pair = flat(pair_ref[span(part)]).astype(jnp.float32)
        open_piece(0, part, pair, norm_out, proj_out)
        if part == 0:
            pl.semaphore_wait(barrier, chips)
        pass_on(0, line, part, start)
    left_out[...] = split(gated(dot(normed_ref[...], proj_out[:, : 2 * hidden])))
    left_copy.start()
    left_f32[0] = left_out[...].astype(jnp.float32)
    gating[...] = jax.nn.sigmoid(dot(normed_ref[...], gate_out[...]))
    left_copy.wait_recv()
    left_f32[1] = left_in[...].astype(jnp.float32)
    exchange(0, outgoing_block)
    part_out[0, :, :share] = partial[1, :, :share].astype(jnp.bfloat16)
    tri_copy.start()
    tri_copy.wait_recv()
    partial[1, :, :share] = part_in[0, :, :share].astype(jnp.float32)
    for half in range(CORES):
        for block in range(chips):
            at = (block * CORES + half) * rows
            got = pl.ds(block * rows, rows)
            tri[:, at : at + rows, :] = jnp.where(
                core == half, partial[0, :, got, :], partial[1, :, got, :]
            )
    for part in range(pieces):
        pair = flat(pair_ref[span(part)]).astype(jnp.float32)
        first = close(pair, part, mid_out, final_out)
        out_ref[span(part)] = first.reshape(piece, tokens, channels)
        open_piece(1, part, first.astype(jnp.float32), norm_in, proj_in)
        pass_on(1, line, part, start)
    left_f32[0] = split(gated(dot(normed_ref[...], proj_in[:, : 2 * hidden]))).astype(jnp.float32)
    columns_f32[...] = jnp.zeros_like(columns_f32)
    for target in range(chips):
        for l in range(rows):
            columns_f32[target, l * pad : l * pad + both, :] = left_f32[
                0, l, target * both : (target + 1) * both, :
            ]
    columns_out[...] = columns_f32[...].astype(jnp.bfloat16)
    for offset in range(1, chips):
        columns_copy(chip, lax.rem(chip + offset, chips)).start()
    columns_in[chip] = columns_out[chip]
    gating[...] = jax.nn.sigmoid(dot(normed_ref[...], gate_in[...]))
    partial[...] = jnp.zeros_like(partial)
    exchange(1, incoming_block)
    part_out[1] = partial[1 - core].astype(jnp.bfloat16)
    sum_copy.start()
    sum_copy.wait_recv()
    tri[...] = partial[core] + part_in[1].astype(jnp.float32)
    for part in range(pieces):
        again = flat(out_ref[span(part)]).astype(jnp.float32)
        out_ref[span(part)] = close(again, part, mid_in, final_in).reshape(piece, tokens, channels)

    for offset in range(1, chips):
        columns_copy(chip, lax.rem(chip + offset, chips)).wait_send()
    left_copy.wait_send()
    tri_copy.wait_send()
    sum_copy.wait_send()
    finish_sends(0)
    finish_sends(1)


def gather_rows(devices, pair_rep, *weights):
    rows, tokens, channels = pair_rep.shape
    hidden = weights[1].shape[1] // 4
    gains = [w.reshape(1, -1) if w.ndim == 1 else w for w in weights]
    chips = devices // CORES
    packed = -(-CORES * rows * rows // 16) * 16
    pieces = 2 if rows % 2 == 0 else 1
    block = (rows, tokens, hidden)
    return pl.pallas_call(
        functools.partial(gather_kernel, devices, pieces),
        out_shape=jax.ShapeDtypeStruct(pair_rep.shape, pair_rep.dtype),
        in_specs=[pl.BlockSpec(memory_space=pltpu.VMEM)] * 11,
        out_specs=pl.BlockSpec(memory_space=pltpu.VMEM),
        scratch_shapes=[
            pltpu.VMEM((2, chips) + block, jnp.bfloat16),
            pltpu.VMEM((chips, packed, hidden), jnp.bfloat16),
            pltpu.VMEM((chips, packed, hidden), jnp.bfloat16),
            pltpu.VMEM((chips, packed, hidden), jnp.float32),
            pltpu.VMEM((packed, hidden), jnp.float32),
            pltpu.VMEM(block, jnp.bfloat16),
            pltpu.VMEM(block, jnp.bfloat16),
            pltpu.VMEM((CORES,) + block, jnp.float32),
            pltpu.VMEM((CORES,) + block, jnp.float32),
            pltpu.VMEM(block, jnp.float32),
            pltpu.VMEM((2,) + block, jnp.bfloat16),
            pltpu.VMEM((2,) + block, jnp.bfloat16),
            pltpu.VMEM((rows * tokens, channels), jnp.float32),
            pltpu.VMEM((rows * tokens, channels), jnp.bfloat16),
            pltpu.SemaphoreType.DMA((2, 3, chips, pieces)),
            pltpu.SemaphoreType.DMA((2, chips, pieces)),
            pltpu.SemaphoreType.DMA((chips,)),
            pltpu.SemaphoreType.DMA((chips,)),
            pltpu.SemaphoreType.DMA((3,)),
            pltpu.SemaphoreType.DMA((3,)),
        ],
        compiler_params=pltpu.CompilerParams(
            collective_id=0, has_side_effects=True, vmem_limit_bytes=VMEM_BYTES
        ),
        name="gather_rows",
    )(pair_rep, *gains)


def exchange_channels(
    pair_rep,
    norm_out,
    proj_out,
    gate_out,
    mid_out,
    final_out,
    norm_in,
    proj_in,
    gate_in,
    mid_in,
    final_in,
):
    first = update(pair_rep, norm_out, proj_out, gate_out, mid_out, final_out, True)
    return update(first, norm_in, proj_in, gate_in, mid_in, final_in, False)


def solution(mesh):
    devices = mesh.shape["axial"]

    def on_device(*arrays):
        if fits(devices, arrays[0].shape, arrays[2].shape):
            return gather_rows(devices, *arrays)
        return exchange_channels(*arrays)

    placed = (P(("groups", "axial"), None, None), P(), P(), P(), P(), P(), P(), P(), P(), P(), P())
    return jax.shard_map(
        on_device,
        mesh=mesh,
        in_specs=placed,
        out_specs=P(("groups", "axial"), None, None),
        check_vma=False,
    )
```

```python
import functools

import jax
import jax.numpy as jnp
from jax import lax
from jax.experimental import pallas as pl
from jax.experimental.pallas import tpu as pltpu
from jax.sharding import PartitionSpec as P

EPS = 1e-05


def normalize(values, gain, axis):
    average = jnp.mean(values, axis=axis, keepdims=True)
    spread = jnp.mean(jnp.square(values - average), axis=axis, keepdims=True)
    return (values - average) * lax.rsqrt(spread + EPS) * gain


def channel_product(left_side, right_side, outgoing):
    formula = "kil,kjl->kij" if outgoing else "kli,klj->kij"
    got_left, got_right = (
        lax.all_to_all(left_side, "axial", split_axis=0, concat_axis=1, tiled=True),
        lax.all_to_all(right_side, "axial", split_axis=0, concat_axis=1, tiled=True),
    )
    return jnp.einsum(formula, got_left, got_right, preferred_element_type=jnp.float32)


def update(pair_rep, norm_gain, weights, gate_weight, mid_gain, final_weight, outgoing):
    normed = normalize(pair_rep.astype(jnp.float32), norm_gain, -1).astype(jnp.bfloat16)
    projected = jnp.einsum("rnc,ck->krn", normed, weights, preferred_element_type=jnp.float32)
    hidden = weights.shape[1] // 4
    left_side = (jax.nn.sigmoid(projected[hidden : 2 * hidden]) * projected[:hidden]).astype(
        jnp.bfloat16
    )
    right_side = (
        jax.nn.sigmoid(projected[3 * hidden :]) * projected[2 * hidden : 3 * hidden]
    ).astype(jnp.bfloat16)
    product = channel_product(left_side, right_side, outgoing)
    tri = lax.all_to_all(
        product.astype(jnp.bfloat16), "axial", split_axis=1, concat_axis=0, tiled=True
    )
    gating = jax.nn.sigmoid(
        jnp.einsum("rnc,ce->rne", normed, gate_weight, preferred_element_type=jnp.float32)
    )
    tri_normed = normalize(tri.astype(jnp.float32), mid_gain[:, None, None], 0).astype(jnp.bfloat16)
    result = jnp.einsum("krn,kc->rnc", tri_normed, final_weight, preferred_element_type=jnp.float32)
    return (pair_rep.astype(jnp.float32) + gating * result).astype(jnp.bfloat16)


MESH = pl.DeviceIdType.MESH
CORES = 2
SIDES = 2
UP, DOWN, ACROSS = range(3)
VMEM_BYTES = 56 * 1024 * 1024


def fits(devices, pair_shape, proj_shape):
    rows, tokens, channels = pair_shape
    hidden = proj_shape[1] // 4
    held = 2 * devices * rows * tokens * hidden * 2
    work = 12 * rows * tokens * max(hidden, channels) * 4
    return (
        devices % (CORES * SIDES) == 0
        and devices * rows == tokens
        and rows <= 8
        and tokens % (16 * CORES) == 0
        and channels == hidden
        and hidden % 128 == 0
        and held + work < VMEM_BYTES // 2
    )


def layer_norm(values, gain):
    average = jnp.mean(values, axis=-1, keepdims=True)
    centred = values - average
    spread = jnp.mean(jnp.square(centred), axis=-1, keepdims=True)
    return centred * lax.rsqrt(spread + EPS) * gain


def dot(left, right):
    return jnp.dot(left, right, preferred_element_type=jnp.float32)


def gather_kernel(
    devices,
    pieces,
    pair_ref,
    norm_out,
    proj_out,
    gate_out,
    mid_out,
    final_out,
    norm_in,
    proj_in,
    gate_in,
    mid_in,
    final_in,
    out_ref,
    held,
    columns_out,
    columns_in,
    columns_f32,
    rows_f32,
    left_out,
    left_in,
    left_f32,
    partial,
    tri,
    part_out,
    part_in,
    gating,
    normed_ref,
    send_sem,
    recv_sem,
    columns_send_sem,
    columns_recv_sem,
    peer_send_sem,
    peer_recv_sem,
):
    rows, tokens, channels = pair_ref.shape
    hidden = held.shape[-1]
    chips = devices // CORES
    length = chips // SIDES
    both = CORES * rows
    pad = both
    share = chips * rows
    piece = rows // pieces
    me = lax.axis_index("axial")
    core = me % CORES
    chip = me // CORES
    side = chip % SIDES
    line = chip // SIDES
    low = jnp.minimum(line, length - 1 - line)

    def near(step):
        if step == 0:
            return line
        first = jnp.where(2 * line < length, 1, -1)
        hop = (step + 1) // 2
        pair = line - first * hop if step % 2 else line + first * hop
        alone = jnp.where(2 * line < length, step, length - 1 - step)
        return jnp.where(step <= 2 * low, pair, alone)

    def index(chip_at):
        return chip_at * CORES + core

    order = [near(step) for step in range(length)]
    mine = [at * SIDES + side for at in order]
    beside = [at * SIDES + 1 - side for at in order]
    peer = chip * CORES + 1 - core
    targets = {
        UP: index(jnp.minimum(line + 1, length - 1) * SIDES + side),
        DOWN: index(jnp.maximum(line - 1, 0) * SIDES + side),
        ACROSS: index(line * SIDES + 1 - side),
    }

    def line_event(event):
        step, part = 1 + event // pieces, event % pieces
        at = order[step]
        if event < 2 * pieces and length > 2:
            inner = low >= 1
            at = jnp.where(inner, order[1 + event % 2], at)
            part = jnp.where(inner, event // 2, part)
        return at, part

    def copy(phase, way, block, part):
        window = pl.ds(part * piece, piece)
        return pltpu.make_async_remote_copy(
            src_ref=held.at[phase, block, window],
            dst_ref=held.at[phase, block, window],
            send_sem=send_sem.at[phase, way, block, part],
            recv_sem=recv_sem.at[phase, block, part],
            device_id={"axial": targets[way]},
            device_id_type=MESH,
        )

    def pass_on(phase, at, part, act):
        block = at * SIDES + side

        @pl.when(jnp.logical_and(at <= line, line < length - 1))
        def _():
            act(copy(phase, UP, block, part))

        @pl.when(jnp.logical_and(at >= line, line > 0))
        def _():
            act(copy(phase, DOWN, block, part))

        act(copy(phase, ACROSS, block, part))

    def start(descriptor):
        descriptor.start()

    def finish_send(descriptor):
        descriptor.wait_send()

    def arrived(phase, block, part):
        copy(phase, ACROSS, block, part).wait_recv()

    def columns_copy(block, target):
        return pltpu.make_async_remote_copy(
            src_ref=columns_out.at[target],
            dst_ref=columns_in.at[block],
            send_sem=columns_send_sem.at[target],
            recv_sem=columns_recv_sem.at[block],
            device_id={"axial": index(target)},
            device_id_type=MESH,
        )

    def peer_copy(source, target, which):
        return pltpu.make_async_remote_copy(
            src_ref=source,
            dst_ref=target,
            send_sem=peer_send_sem.at[which],
            recv_sem=peer_recv_sem.at[which],
            device_id={"axial": peer},
            device_id_type=MESH,
        )

    left_copy = peer_copy(left_out, left_in, 0)
    tri_copy = peer_copy(part_out.at[0, :, :share], part_in.at[0, :, :share], 1)
    sum_copy = peer_copy(part_out.at[1], part_in.at[1], 2)

    def exchange(phase, multiply):
        def from_line(step):
            for event in range((step - 1) * pieces, step * pieces):
                at, part = line_event(event)
                arrived(phase, at * SIDES + side, part)
                pass_on(phase, at, part, start)

        def from_side(step):
            for part in range(pieces):
                arrived(phase, beside[step], part)
            multiply(beside[step])

        multiply(mine[0])
        for step in range(1, length):
            from_line(step)
            if step == 2:
                from_side(0)
            if 2 <= step < length - 1:
                multiply(mine[step - 1])
        for step in range(max(1, length - 2), length):
            multiply(mine[step])
        for step in range(1 if length > 2 else 0, length):
            from_side(step)

    def finish_sends(phase):
        for step in range(length):
            for part in range(pieces):
                pass_on(phase, order[step], part, finish_send)

    def split(values):
        return values.reshape(rows, tokens, values.shape[-1])

    def gated(projected):
        return (jax.nn.sigmoid(projected[:, hidden:]) * projected[:, :hidden]).astype(jnp.bfloat16)

    def outgoing_block(block):
        def one(row, carry):
            right = held[0, block, row].astype(jnp.float32)
            at = pl.ds(block * rows + row, 1)
            for half in range(CORES):
                total = jnp.sum(left_f32[half] * right[None], axis=1, keepdims=True)
                partial[half, :, at, :] = total
            return carry

        lax.fori_loop(0, rows, one, 0)

    def incoming_block(block):
        @pl.when(block != chip)
        def _():
            columns_copy(block, chip * 0 + beside[0]).wait_recv()

        rows_f32[...] = columns_in[block].astype(jnp.float32)

        def one(tile, carry):
            window = pl.ds(pl.multiple_of(tile * 16, 16), 16)
            right = held[1, block, :, window, :].astype(jnp.float32)
            for i in range(both):
                total = partial[i // rows, i % rows, window, :]
                for l in range(rows):
                    total = total + rows_f32[pl.ds(l * pad + i, 1), :] * right[l]
                partial[i // rows, i % rows, window, :] = total
            return carry

        lax.fori_loop(0, tokens // 16, one, 0)

    def flat(values):
        return values.reshape(-1, values.shape[-1])

    def close(pair, part, mid_gain, final):
        product = flat(tri[span(part)]).astype(jnp.bfloat16).astype(jnp.float32)
        normed = layer_norm(product, mid_gain[...]).astype(jnp.bfloat16)
        return (pair + gating[flat_span(part)] * dot(normed, final[...])).astype(jnp.bfloat16)

    def span(part):
        return pl.ds(part * piece, piece)

    def flat_span(part):
        return pl.ds(part * piece * tokens, piece * tokens)

    def open_piece(phase, part, pair, norm, proj):
        normed = layer_norm(pair, norm[...]).astype(jnp.bfloat16)
        normed_ref[flat_span(part)] = normed
        right = gated(dot(normed, proj[:, 2 * hidden :]))
        held[phase, chip, span(part)] = right.reshape(piece, tokens, hidden)

    barrier = pltpu.get_barrier_semaphore()
    for offset in range(1, chips):
        pl.semaphore_signal(
            barrier,
            inc=1,
            device_id={"axial": index(lax.rem(chip + offset, chips))},
            device_id_type=MESH,
        )
    pl.semaphore_signal(barrier, inc=1, device_id={"axial": peer}, device_id_type=MESH)

    for part in range(pieces):
        pair = flat(pair_ref[span(part)]).astype(jnp.float32)
        open_piece(0, part, pair, norm_out, proj_out)
        if part == 0:
            pl.semaphore_wait(barrier, chips)
        pass_on(0, line, part, start)
    left_out[...] = split(gated(dot(normed_ref[...], proj_out[:, : 2 * hidden])))
    left_copy.start()
    left_f32[0] = left_out[...].astype(jnp.float32)
    gating[...] = jax.nn.sigmoid(dot(normed_ref[...], gate_out[...]))
    left_copy.wait_recv()
    left_f32[1] = left_in[...].astype(jnp.float32)
    exchange(0, outgoing_block)
    part_out[0, :, :share] = partial[1, :, :share].astype(jnp.bfloat16)
    tri_copy.start()
    tri_copy.wait_recv()
    partial[1, :, :share] = part_in[0, :, :share].astype(jnp.float32)
    for half in range(CORES):
        for block in range(chips):
            at = (block * CORES + half) * rows
            got = pl.ds(block * rows, rows)
            tri[:, at : at + rows, :] = jnp.where(
                core == half, partial[0, :, got, :], partial[1, :, got, :]
            )
    for part in range(pieces):
        pair = flat(pair_ref[span(part)]).astype(jnp.float32)
        first = close(pair, part, mid_out, final_out)
        out_ref[span(part)] = first.reshape(piece, tokens, channels)
        open_piece(1, part, first.astype(jnp.float32), norm_in, proj_in)
        pass_on(1, line, part, start)
    left_f32[0] = split(gated(dot(normed_ref[...], proj_in[:, : 2 * hidden]))).astype(jnp.float32)
    columns_f32[...] = jnp.zeros_like(columns_f32)
    for target in range(chips):
        for l in range(rows):
            columns_f32[target, l * pad : l * pad + both, :] = left_f32[
                0, l, target * both : (target + 1) * both, :
            ]
    columns_out[...] = columns_f32[...].astype(jnp.bfloat16)
    for offset in range(1, chips):
        columns_copy(chip, lax.rem(chip + offset, chips)).start()
    columns_in[chip] = columns_out[chip]
    gating[...] = jax.nn.sigmoid(dot(normed_ref[...], gate_in[...]))
    partial[...] = jnp.zeros_like(partial)
    exchange(1, incoming_block)
    part_out[1] = partial[1 - core].astype(jnp.bfloat16)
    sum_copy.start()
    sum_copy.wait_recv()
    tri[...] = partial[core] + part_in[1].astype(jnp.float32)
    for part in range(pieces):
        again = flat(out_ref[span(part)]).astype(jnp.float32)
        out_ref[span(part)] = close(again, part, mid_in, final_in).reshape(piece, tokens, channels)

    for offset in range(1, chips):
        columns_copy(chip, lax.rem(chip + offset, chips)).wait_send()
    left_copy.wait_send()
    tri_copy.wait_send()
    sum_copy.wait_send()
    finish_sends(0)
    finish_sends(1)


def gather_rows(devices, pair_rep, *weights):
    rows, tokens, channels = pair_rep.shape
    hidden = weights[1].shape[1] // 4
    gains = [w.reshape(1, -1) if w.ndim == 1 else w for w in weights]
    chips = devices // CORES
    packed = -(-CORES * rows * rows // 16) * 16
    pieces = next(count for count in (3, 2, 1) if rows % count == 0)
    block = (rows, tokens, hidden)
    return pl.pallas_call(
        functools.partial(gather_kernel, devices, pieces),
        out_shape=jax.ShapeDtypeStruct(pair_rep.shape, pair_rep.dtype),
        in_specs=[pl.BlockSpec(memory_space=pltpu.VMEM)] * 11,
        out_specs=pl.BlockSpec(memory_space=pltpu.VMEM),
        scratch_shapes=[
            pltpu.VMEM((2, chips) + block, jnp.bfloat16),
            pltpu.VMEM((chips, packed, hidden), jnp.bfloat16),
            pltpu.VMEM((chips, packed, hidden), jnp.bfloat16),
            pltpu.VMEM((chips, packed, hidden), jnp.float32),
            pltpu.VMEM((packed, hidden), jnp.float32),
            pltpu.VMEM(block, jnp.bfloat16),
            pltpu.VMEM(block, jnp.bfloat16),
            pltpu.VMEM((CORES,) + block, jnp.float32),
            pltpu.VMEM((CORES,) + block, jnp.float32),
            pltpu.VMEM(block, jnp.float32),
            pltpu.VMEM((2,) + block, jnp.bfloat16),
            pltpu.VMEM((2,) + block, jnp.bfloat16),
            pltpu.VMEM((rows * tokens, channels), jnp.float32),
            pltpu.VMEM((rows * tokens, channels), jnp.bfloat16),
            pltpu.SemaphoreType.DMA((2, 3, chips, pieces)),
            pltpu.SemaphoreType.DMA((2, chips, pieces)),
            pltpu.SemaphoreType.DMA((chips,)),
            pltpu.SemaphoreType.DMA((chips,)),
            pltpu.SemaphoreType.DMA((3,)),
            pltpu.SemaphoreType.DMA((3,)),
        ],
        compiler_params=pltpu.CompilerParams(
            collective_id=0, has_side_effects=True, vmem_limit_bytes=VMEM_BYTES
        ),
        name="gather_rows",
    )(pair_rep, *gains)


def exchange_channels(
    pair_rep,
    norm_out,
    proj_out,
    gate_out,
    mid_out,
    final_out,
    norm_in,
    proj_in,
    gate_in,
    mid_in,
    final_in,
):
    first = update(pair_rep, norm_out, proj_out, gate_out, mid_out, final_out, True)
    return update(first, norm_in, proj_in, gate_in, mid_in, final_in, False)


def solution(mesh):
    devices = mesh.shape["axial"]

    def on_device(*arrays):
        if fits(devices, arrays[0].shape, arrays[2].shape):
            return gather_rows(devices, *arrays)
        return exchange_channels(*arrays)

    placed = (P(("groups", "axial"), None, None), P(), P(), P(), P(), P(), P(), P(), P(), P(), P())
    return jax.shard_map(
        on_device,
        mesh=mesh,
        in_specs=placed,
        out_specs=P(("groups", "axial"), None, None),
        check_vma=False,
    )
```
